32 devices in a mesh: group: 2 (over y), tm: 4 (over z), bl: 2 (over x), pol: 2 (over core).
Axes of the slice: x: 2, y: 2, z: 4, core: 2. Of those that a mesh axis runs over, the one named last changes fastest.
Arguments:
- visibilities: bfloat16 [1600, 256, 2, 384], P(('group', 'tm'), ('bl', 'pol')), parts along dimension 0, may hold values from -6 to 6
- flag_mask: int32 [1600], P(('group', 'tm')), parts along dimension 0, may hold values 0 or 1
- kernel_index: int32 [256], P(('bl', 'pol')), may hold values from 0 to 15
- filter_bank: float32 [2, 16, 257], replicated, may hold values from -0.875 to 0.875
Outputs:
- fringe_filtered: bfloat16 [160, 256, 2, 384], P('group', ('bl', 'pol', 'tm')), parts along dimension 0
The draws below stay inside these ranges and needn't reach their ends.
There are 2 independent parts, one for each index of `group`. The reference program is written for one: setup_inputs(seed, part) draws one part's arguments, and reference() takes and returns one part's arrays. A program takes and returns all parts, laid end to end along the dimension named above; an argument that names none is the same for every part. Nothing has to cross between parts.
All inputs are finite; a program needn't handle non-finite values. No bound on the sum of `flag_mask` on one device may be relied on, other than what follows from the above.
Results may differ from the reference program's by a relative error of at most 0.001.
Values may be sent and summed in bfloat16 or wider, within the bound.
A program may use at most 192 MiB of HBM per device.

```python
import jax
import jax.numpy as jnp
from jax import lax

BASE = 256
CHAN = 384
TAPS = 257
AVG = 10
NKERN = 16
T_DEV = 200
TIMES = 800
OUT_TIMES = 80


def place_ends(array, stream_key, least, top_value):
    index_at = [jax.random.randint(jax.random.fold_in(stream_key, axis), (), 0, length) for axis, length in enumerate(array.shape)]
    widest = array.shape.index(max(array.shape))
    neighbour = index_at[:widest] + [(index_at[widest] + 1) % array.shape[widest]] + index_at[widest + 1:]
    return array.at[tuple(index_at)].set(least).at[tuple(neighbour)].set(top_value)


def block_levels(own_key, shape, shards, smallest, largest):
    level, own = 1.0, jax.random.fold_in(own_key, 6)
    for position, shards_of in shards:
        draws = jnp.exp(jax.random.uniform(jax.random.fold_in(own, position), (shards_of,), jnp.float32, smallest / len(shards), largest / len(shards)))
        level = level * jnp.repeat(draws, shape[position] // shards_of).reshape([-1 if axis == position else 1 for axis in range(len(shape))])
    return level


def gaussian(own_key, shape, scale, limit, pieces=(), kind=jnp.bfloat16):
    factor_of = block_levels(own_key, shape, pieces, -0.22, 0.18) if pieces else 1.0
    entries = jax.random.normal(own_key, shape, jnp.float32) * scale * factor_of
    return jnp.minimum(jnp.maximum(entries, -limit), limit).astype(kind)


def setup_inputs(seed: int = 0, part: int = 0) -> dict:
    keys = jax.random.split(jax.random.key(seed), 5)
    part_splits = jax.random.split(jax.random.fold_in(keys[4], part), 5)
    visibilities = gaussian(part_splits[0], (TIMES, BASE, 2, CHAN), 1.0, 6.0, ((0, 4), (1, 4)))
    flag_mask = place_ends((jax.random.randint(part_splits[1], (TIMES,), 0, 10) < 9).astype(jnp.int32), jax.random.fold_in(part_splits[1], 1), 0, 1)
    kernel_index = place_ends(jax.random.randint(keys[2], (BASE,), 0, NKERN), jax.random.fold_in(keys[2], 1), 0, NKERN - 1).astype(jnp.int32)
    filter_bank = gaussian(keys[3], (2, NKERN, TAPS), (TAPS // 5) ** -0.5, 0.875, (), jnp.float32)
    return {"visibilities": visibilities, "flag_mask": flag_mask, "kernel_index": kernel_index, "filter_bank": filter_bank}


def select_taps(kernel_index, filter_bank):
    choices_count = filter_bank.shape[1]
    one_hot = (kernel_index[:, None] == jnp.arange(choices_count, dtype=jnp.int32)[None, :]).astype(jnp.float32)
    return jnp.einsum("bk,rkt->brt", one_hot, filter_bank, precision=lax.Precision.HIGHEST)


def make_band(kernel_taps, block_rows):
    tap_count = kernel_taps.shape[1]
    row_width = block_rows + tap_count - 1
    zero_tail = jnp.zeros((2, block_rows), jnp.float32)
    period_row = jnp.concatenate([kernel_taps, zero_tail], axis=1)
    tiled_rows = jnp.tile(period_row, (1, block_rows))[:, :block_rows * row_width]
    return tiled_rows.reshape(2, block_rows, row_width)


def filter_block(time_slab, kernel_taps, block_rows, joined_average):
    band_rows = make_band(kernel_taps, block_rows)
    row_width = band_rows.shape[2]
    if joined_average:
        band_rows = band_rows.reshape(2, block_rows // AVG, AVG, row_width).sum(axis=2) * (1.0 / AVG)
    out_count = band_rows.shape[1]
    stacked = band_rows.reshape(2 * out_count, row_width)
    product = jnp.dot(stacked, time_slab, precision=lax.Precision.HIGHEST, preferred_element_type=jnp.float32)
    prod_real = product[:out_count]
    prod_imag = product[out_count:]
    channels = time_slab.shape[1] // 2
    out_real = prod_real[:, :channels] - prod_imag[:, channels:]
    out_imag = prod_real[:, channels:] + prod_imag[:, :channels]
    result = jnp.stack([out_real, out_imag], axis=1)
    if not joined_average:
        result = result.reshape(out_count // AVG, AVG, 2, channels).sum(axis=1) * (1.0 / AVG)
    return result


def reference(visibilities, flag_mask, kernel_index, filter_bank):
    half_taps = TAPS // 2
    flag_float = flag_mask.astype(jnp.float32)
    taps_all = select_taps(kernel_index, filter_bank)
    block_count = TIMES // T_DEV

    def per_base(base_index):
        column = lax.dynamic_index_in_dim(visibilities, base_index, 1, False).astype(jnp.float32)
        column = (column * flag_float[:, None, None]).reshape(TIMES, 2 * CHAN)
        padded = jnp.pad(column, ((half_taps, half_taps), (0, 0)))
        kernel_taps = lax.dynamic_index_in_dim(taps_all, base_index, 0, False)

        def per_block(block_index):
            time_slab = lax.dynamic_slice_in_dim(padded, (block_index * T_DEV).astype(jnp.int32), T_DEV + TAPS - 1, 0)
            return filter_block(time_slab, kernel_taps, T_DEV, True)

        blocks_out = lax.map(per_block, jnp.arange(block_count, dtype=jnp.int32))
        return blocks_out.reshape(OUT_TIMES, 2, CHAN)

    filtered = lax.map(per_base, jnp.arange(BASE, dtype=jnp.int32))
    return jnp.moveaxis(filtered, 0, 1).astype(jnp.bfloat16)
```

```python
import functools

import jax
import jax.numpy as jnp
from jax import lax
from jax.experimental import pallas as pl
from jax.experimental.pallas import tpu as pltpu
from jax.sharding import PartitionSpec as P

TAPS = 257
AVG = 10
HALF = TAPS // 2
SIDE = -(-HALF // AVG)
GROUP = 8


def round_up(value, step):
    return -(-value // step) * step


def row_plan(block_rows):
    out_count = block_rows // AVG
    side_rows = round_up(2 * SIDE, 8)
    local_rows = round_up(2 * out_count, 8)
    highest = 2 * (block_rows + HALF + AVG * SIDE)
    lowest = 2 * HALF - AVG * (2 * out_count + side_rows)
    period = round_up(max(highest, 2 * (TAPS + AVG) - lowest), 128)
    return out_count, side_rows, local_rows, period


def averaged_taps(filter_bank, period):
    width = TAPS + AVG - 1
    padded = jnp.pad(filter_bank, ((0, 0), (0, 0), (AVG - 1, AVG - 1)))
    total = padded[:, :, 0:width]
    for shift in range(1, AVG):
        total = total + padded[:, :, shift : shift + width]
    real, imag = total[0] * (1.0 / AVG), total[1] * (1.0 / AVG)
    to_real = jnp.stack([real, -imag], axis=-1).reshape(-1, 2 * width)
    to_imag = jnp.stack([imag, real], axis=-1).reshape(-1, 2 * width)
    to_real = jnp.pad(to_real, ((0, 0), (0, period - 2 * width)))
    to_imag = jnp.pad(to_imag, ((0, 0), (0, period - 2 * width)))
    pair = jnp.stack([to_real, jnp.roll(to_imag, -AVG, axis=1)], axis=1)
    return jnp.tile(pair, (1, 4, 1))


def build_bands(taps_ref, flag_ref, band_ref, block_rows):
    out_count, side_rows, local_rows, period = row_plan(block_rows)
    total_rows = 2 * side_rows + local_rows
    flags = flag_ref[...].astype(jnp.float32)

    def one_filter(f, carry):
        tile = pltpu.roll(taps_ref[f], 0, 1, stride=AVG, stride_axis=0)
        start = 0
        for first, rows in (
            (-2 * SIDE, side_rows),
            (0, local_rows),
            (2 * out_count, side_rows),
        ):
            shifts = [(AVG * (first + row) - 2 * HALF) % period for row in range(0, rows, 8)]
            tiles = [pltpu.roll(tile, shift, 1)[:, : 2 * block_rows] for shift in shifts]
            band = jnp.concatenate(tiles, axis=0) * flags
            high = band.astype(jnp.bfloat16)
            low = (band - high.astype(jnp.float32)).astype(jnp.bfloat16)
            band_ref[f, start : start + rows, :] = high
            band_ref[f, total_rows + start : total_rows + start + rows, :] = low
            start += rows
        return carry

    lax.fori_loop(0, taps_ref.shape[0], one_filter, 0)


def filter_kernel(
    index_ref, taps_ref, flag_ref, vis_ref, left_ref, local_ref, right_ref, band_ref, *, first_base
):
    block_rows, group, _, channels = vis_ref.shape
    out_count, side_rows, local_rows, _ = row_plan(block_rows)
    total_rows = 2 * side_rows + local_rows
    side = 2 * SIDE

    @pl.when(pl.program_id(0) == 0)
    def _():
        build_bands(taps_ref, flag_ref, band_ref, block_rows)

    for i in range(group):
        which = index_ref[first_base + pl.program_id(0) * group + i]
        slab = vis_ref[:, i].reshape(2 * block_rows, channels)
        both = jnp.dot(band_ref[which], slab, preferred_element_type=jnp.float32)
        rows = both[:total_rows] + both[total_rows:]
        left_ref[0, side * i : side * (i + 1), :] = rows[:side]
        local_ref[i] = rows[side_rows : side_rows + 2 * out_count]
        start = side_rows + local_rows
        right_ref[0, side * i : side * (i + 1), :] = rows[start : start + side]


def filter_call(visibilities, flags, kernel_index, taps, first, count, group):
    block_rows, _, _, channels = visibilities.shape
    out_count, side_rows, local_rows, period = row_plan(block_rows)
    filters = taps.shape[0]
    steps = count // group
    skip = first // group
    side_shape = jax.ShapeDtypeStruct((steps, 2 * SIDE * group, channels), jnp.float32)
    side_spec = pl.BlockSpec((1, 2 * SIDE * group, channels), lambda i, _: (i, 0, 0))
    return pl.pallas_call(
        functools.partial(filter_kernel, first_base=first),
        grid_spec=pltpu.PrefetchScalarGridSpec(
            num_scalar_prefetch=1,
            grid=(steps,),
            in_specs=[
                pl.BlockSpec((filters, 8, period), lambda i, _: (0, 0, 0)),
                pl.BlockSpec((1, 2 * block_rows), lambda i, _: (0, 0)),
                pl.BlockSpec((block_rows, group, 2, channels), lambda i, _: (0, skip + i, 0, 0)),
            ],
            out_specs=[
                side_spec,
                pl.BlockSpec((group, 2 * out_count, channels), lambda i, _: (i, 0, 0)),
                side_spec,
            ],
            scratch_shapes=[
                pltpu.VMEM(
                    (filters, 2 * (2 * side_rows + local_rows), 2 * block_rows), jnp.bfloat16
                )
            ],
        ),
        out_shape=[
            side_shape,
            jax.ShapeDtypeStruct((count, 2 * out_count, channels), jnp.float32),
            side_shape,
        ],
        cost_estimate=pl.CostEstimate(
            flops=count * 2 * 208 * 400 * channels,
            bytes_accessed=count * block_rows * 2 * channels * 4,
            transcendentals=0,
        ),
    )(kernel_index, taps, flags, visibilities)


def finish_kernel(low_ref, local_ref, high_ref, out_ref, sum_ref):
    group, rows, channels = local_ref.shape
    side = 2 * SIDE
    for i in range(group):
        sum_ref[...] = local_ref[i]
        sum_ref[:side] += low_ref[0, side * i : side * (i + 1), :]
        sum_ref[rows - side :] += high_ref[0, side * i : side * (i + 1), :]
        out_ref[:, i] = sum_ref[...].astype(jnp.bfloat16).reshape(rows // 2, 2, channels)


def finish_call(low, local, high, group):
    count, rows, channels = local.shape
    side_spec = pl.BlockSpec((1, 2 * SIDE * group, channels), lambda i: (i, 0, 0))
    return pl.pallas_call(
        finish_kernel,
        grid=(count // group,),
        in_specs=[
            side_spec,
            pl.BlockSpec((group, rows, channels), lambda i: (i, 0, 0)),
            side_spec,
        ],
        out_specs=pl.BlockSpec((rows // 2, group, 2, channels), lambda i: (0, i, 0, 0)),
        out_shape=jax.ShapeDtypeStruct((rows // 2, count, 2, channels), jnp.bfloat16),
        scratch_shapes=[pltpu.VMEM((rows, channels), jnp.float32)],
    )(low, local, high)


def per_device(visibilities, flag_mask, kernel_index, filter_bank):
    block_rows, bases = visibilities.shape[:2]
    period = row_plan(block_rows)[3]
    taps = averaged_taps(filter_bank, period)
    flags = jnp.repeat(flag_mask, 2)[None, :]
    group = GROUP
    while bases % group:
        group //= 2
    chunk_count = 4 if bases % (4 * group) == 0 else 1
    chunk = bases // chunk_count
    count = lax.axis_size("tm")
    forward = [(i, i + 1) for i in range(count - 1)]
    backward = [(j, i) for i, j in forward]
    parts = []
    for c in range(chunk_count):
        to_left, local, to_right = filter_call(
            visibilities, flags, kernel_index, taps, c * chunk, chunk, group
        )
        low = lax.ppermute(to_right, "tm", forward)
        high = lax.ppermute(to_left, "tm", backward)
        parts.append((low, local, high))
    done = [finish_call(low, local, high, group) for low, local, high in parts]
    averaged = jnp.concatenate(done, axis=1)
    return lax.all_to_all(averaged, "tm", split_axis=1, concat_axis=0, tiled=True)


def solution(mesh):
    placed = (
        P(("group", "tm"), ("bl", "pol"), None, None),
        P(("group", "tm")),
        P(("bl", "pol")),
        P(),
    )
    return jax.shard_map(
        per_device,
        mesh=mesh,
        in_specs=placed,
        out_specs=P("group", ("bl", "pol", "tm"), None, None),
        check_vma=False,
    )
```

```python
import functools

import jax
import jax.numpy as jnp
from jax import lax
from jax.experimental import pallas as pl
from jax.experimental.pallas import tpu as pltpu
from jax.sharding import PartitionSpec as P

TAPS = 257
AVG = 10
HALF = TAPS // 2
SIDE = -(-HALF // AVG)
GROUP = 8


def round_up(value, step):
    return -(-value // step) * step


def row_plan(block_rows):
    out_count = block_rows // AVG
    side_rows = round_up(2 * SIDE, 8)
    local_rows = round_up(2 * out_count, 8)
    highest = 2 * (block_rows + HALF + AVG * SIDE)
    lowest = 2 * HALF - AVG * (2 * out_count + side_rows)
    period = round_up(max(highest, 2 * (TAPS + AVG) - lowest), 128)
    return out_count, side_rows, local_rows, period


def averaged_taps(filter_bank, period):
    width = TAPS + AVG - 1
    padded = jnp.pad(filter_bank, ((0, 0), (0, 0), (AVG - 1, AVG - 1)))
    total = padded[:, :, 0:width]
    for shift in range(1, AVG):
        total = total + padded[:, :, shift : shift + width]
    real, imag = total[0] * (1.0 / AVG), total[1] * (1.0 / AVG)
    to_real = jnp.stack([real, -imag], axis=-1).reshape(-1, 2 * width)
    to_imag = jnp.stack([imag, real], axis=-1).reshape(-1, 2 * width)
    to_real = jnp.pad(to_real, ((0, 0), (0, period - 2 * width)))
    to_imag = jnp.pad(to_imag, ((0, 0), (0, period - 2 * width)))
    pair = jnp.stack([to_real, jnp.roll(to_imag, -AVG, axis=1)], axis=1)
    return jnp.tile(pair, (1, 4, 1))


def build_bands(taps_ref, flag_ref, band_ref, block_rows):
    out_count, side_rows, local_rows, period = row_plan(block_rows)
    total_rows = 2 * side_rows + local_rows
    flags = flag_ref[...].astype(jnp.float32)

    def one_filter(f, carry):
        tile = pltpu.roll(taps_ref[f], 0, 1, stride=AVG, stride_axis=0)
        start = 0
        for first, rows in (
            (-2 * SIDE, side_rows),
            (0, local_rows),
            (2 * out_count, side_rows),
        ):
            shifts = [(AVG * (first + row) - 2 * HALF) % period for row in range(0, rows, 8)]
            tiles = [pltpu.roll(tile, shift, 1)[:, : 2 * block_rows] for shift in shifts]
            band = jnp.concatenate(tiles, axis=0) * flags
            high = band.astype(jnp.bfloat16)
            low = (band - high.astype(jnp.float32)).astype(jnp.bfloat16)
            band_ref[f, start : start + rows, :] = high
            band_ref[f, total_rows + start : total_rows + start + rows, :] = low
            start += rows
        return carry

    lax.fori_loop(0, taps_ref.shape[0], one_filter, 0)


def band_kernel(taps_ref, flag_ref, band_ref, *, block_rows):
    build_bands(taps_ref, flag_ref, band_ref, block_rows)


def band_call(taps, flags):
    block_rows = flags.shape[1] // 2
    _, side_rows, local_rows, _ = row_plan(block_rows)
    return pl.pallas_call(
        functools.partial(band_kernel, block_rows=block_rows),
        in_specs=[pl.BlockSpec(memory_space=pltpu.VMEM)] * 2,
        out_specs=pl.BlockSpec(memory_space=pltpu.VMEM),
        out_shape=jax.ShapeDtypeStruct(
            (taps.shape[0], 2 * (2 * side_rows + local_rows), 2 * block_rows), jnp.bfloat16
        ),
    )(taps, flags)


def stream_kernel(
    index_ref,
    band_ref,
    vis_ref,
    out_ref,
    slab_ref,
    to_left,
    to_right,
    from_left,
    from_right,
    local_ref,
    sum_ref,
    done_ref,
    load_sem,
    left_send,
    right_send,
    left_recv,
    right_recv,
    done_send,
    done_recv,
    *,
    count,
):
    me = lax.axis_index("tm")
    _, block_rows, group, _, channels = slab_ref.shape
    chunks = done_ref.shape[0]
    per_owner = chunks // count
    out_count, side_rows, local_rows, _ = row_plan(block_rows)
    total_rows = 2 * side_rows + local_rows
    side = 2 * SIDE
    has_left, has_right = me > 0, me < count - 1

    def chunk_at(step):
        turn = step % count
        owner = (turn % 2) * (count - 1 - turn // 2) + (1 - turn % 2) * (turn // 2)
        return owner, step // count

    def load(step):
        owner, part = chunk_at(step)
        first = (owner * per_owner + part) * group
        slot = step % 2
        return pltpu.make_async_copy(
            vis_ref.at[:, pl.ds(first, group)], slab_ref.at[slot], load_sem.at[slot]
        )

    def remote(source, target, send_sem, recv_sem, device):
        return pltpu.make_async_remote_copy(
            src_ref=source,
            dst_ref=target,
            send_sem=send_sem,
            recv_sem=recv_sem,
            device_id={"tm": device},
            device_id_type=pl.DeviceIdType.MESH,
        )

    def leftward(step):
        return remote(
            to_left.at[step],
            from_right.at[step],
            left_send.at[step],
            right_recv.at[step],
            jnp.maximum(me - 1, 0),
        )

    def rightward(step):
        return remote(
            to_right.at[step],
            from_left.at[step],
            right_send.at[step],
            left_recv.at[step],
            jnp.minimum(me + 1, count - 1),
        )

    def placed(source, part):
        return out_ref.at[pl.ds(source * out_count, out_count), pl.ds(part * group, group)]

    def deliver(step):
        owner, part = chunk_at(step)
        return remote(
            done_ref.at[step], placed(me, part), done_send.at[step], done_recv.at[me, part], owner
        )

    def keep(step):
        _, part = chunk_at(step)
        return pltpu.make_async_copy(done_ref.at[step], placed(me, part), done_send.at[step])

    load(0).start()
    barrier = pltpu.get_barrier_semaphore()
    for offset in range(1, count):
        pl.semaphore_signal(
            barrier,
            inc=1,
            device_id={"tm": lax.rem(me + offset, count)},
            device_id_type=pl.DeviceIdType.MESH,
        )
    pl.semaphore_wait(barrier, count - 1)

    def compute(step, carry):
        @pl.when(step + 1 < chunks)
        def _():
            load(step + 1).start()

        load(step).wait()
        owner, part = chunk_at(step)
        first = (owner * per_owner + part) * group
        slot = step % 2
        for i in range(group):
            which = index_ref[first + i]
            slab = slab_ref[slot, :, i].reshape(2 * block_rows, channels)
            both = jnp.dot(band_ref[which], slab, preferred_element_type=jnp.float32)
            rows = both[:total_rows] + both[total_rows:]
            to_left[step, side * i : side * (i + 1), :] = rows[:side]
            local_ref[step, i] = rows[side_rows : side_rows + 2 * out_count]
            start = side_rows + local_rows
            to_right[step, side * i : side * (i + 1), :] = rows[start : start + side]

        @pl.when(has_left)
        def _():
            leftward(step).start()

        @pl.when(has_right)
        def _():
            rightward(step).start()

        return carry

    lax.fori_loop(0, chunks, compute, 0)

    def finish(step, carry):
        @pl.when(has_left)
        def _():
            rightward(step).wait_recv()

        @pl.when(has_right)
        def _():
            leftward(step).wait_recv()

        for i in range(group):
            sum_ref[...] = local_ref[step, i]

            @pl.when(has_left)
            def _():
                sum_ref[:side] += from_left[step, side * i : side * (i + 1), :]

            @pl.when(has_right)
            def _():
                sum_ref[2 * out_count - side :] += from_right[step, side * i : side * (i + 1), :]

            done_ref[step, :, i] = (
                sum_ref[...].astype(jnp.bfloat16).reshape(out_count, 2, channels)
            )
        owner, _ = chunk_at(step)

        @pl.when(owner == me)
        def _():
            keep(step).start()

        @pl.when(owner != me)
        def _():
            deliver(step).start()

        return carry

    lax.fori_loop(0, chunks, finish, 0)

    def drain(step, carry):
        @pl.when(has_left)
        def _():
            leftward(step).wait_send()

        @pl.when(has_right)
        def _():
            rightward(step).wait_send()

        owner, _ = chunk_at(step)

        @pl.when(owner == me)
        def _():
            keep(step).wait()

        @pl.when(owner != me)
        def _():
            deliver(step).wait_send()

        return carry

    lax.fori_loop(0, chunks, drain, 0)

    def collect(turn, carry):
        source = lax.rem(me + 1 + turn, count)
        for part in range(per_owner):
            remote(
                done_ref.at[0],
                placed(source, part),
                done_send.at[0],
                done_recv.at[source, part],
                source,
            ).wait_recv()
        return carry

    lax.fori_loop(0, count - 1, collect, 0)


def stream_call(kernel_index, bands, visibilities):
    block_rows, bases, _, channels = visibilities.shape
    count = lax.axis_size("tm")
    out_count = block_rows // AVG
    owned = bases // count
    group = GROUP
    while owned % group:
        group //= 2
    chunks = bases // group
    edge = pltpu.VMEM((chunks, 2 * SIDE * group, channels), jnp.float32)
    chunk_sems = pltpu.SemaphoreType.DMA((chunks,))
    return pl.pallas_call(
        functools.partial(stream_kernel, count=count),
        in_specs=[
            pl.BlockSpec(memory_space=pltpu.SMEM),
            pl.BlockSpec(memory_space=pltpu.VMEM),
            pl.BlockSpec(memory_space=pl.ANY),
        ],
        out_specs=pl.BlockSpec(memory_space=pl.ANY),
        out_shape=jax.ShapeDtypeStruct((count * out_count, owned, 2, channels), jnp.bfloat16),
        scratch_shapes=[
            pltpu.VMEM((2, block_rows, group, 2, channels), jnp.bfloat16),
            edge,
            edge,
            edge,
            edge,
            pltpu.VMEM((chunks, group, 2 * out_count, channels), jnp.float32),
            pltpu.VMEM((2 * out_count, channels), jnp.float32),
            pltpu.VMEM((chunks, out_count, group, 2, channels), jnp.bfloat16),
            pltpu.SemaphoreType.DMA((2,)),
            chunk_sems,
            chunk_sems,
            chunk_sems,
            chunk_sems,
            chunk_sems,
            pltpu.SemaphoreType.DMA((count, owned // group)),
        ],
        compiler_params=pltpu.CompilerParams(
            collective_id=0, has_side_effects=True, vmem_limit_bytes=50 * 1024 * 1024
        ),
    )(kernel_index, bands, visibilities)


def per_device(visibilities, flag_mask, kernel_index, filter_bank):
    period = row_plan(visibilities.shape[0])[3]
    taps = averaged_taps(filter_bank, period)
    flags = jnp.repeat(flag_mask, 2)[None, :]
    bands = band_call(taps, flags)
    return stream_call(kernel_index, bands, visibilities)


def solution(mesh):
    placed = (
        P(("group", "tm"), ("bl", "pol"), None, None),
        P(("group", "tm")),
        P(("bl", "pol")),
        P(),
    )
    return jax.shard_map(
        per_device,
        mesh=mesh,
        in_specs=placed,
        out_specs=P("group", ("bl", "pol", "tm"), None, None),
        check_vma=False,
    )
```

```python
import functools

import jax
import jax.numpy as jnp
from jax import lax
from jax.experimental import pallas as pl
from jax.experimental.pallas import tpu as pltpu
from jax.sharding import PartitionSpec as P

TAPS = 257
AVG = 10
HALF = TAPS // 2
SIDE = -(-HALF // AVG)
GROUP = 8


def round_up(value, step):
    return -(-value // step) * step


def row_plan(block_rows):
    out_count = block_rows // AVG
    side_rows = round_up(2 * SIDE, 8)
    local_rows = round_up(2 * out_count, 8)
    highest = 2 * (block_rows + HALF + AVG * SIDE)
    lowest = 2 * HALF - AVG * (2 * out_count + side_rows)
    period = round_up(max(highest, 2 * (TAPS + AVG) - lowest), 128)
    return out_count, side_rows, local_rows, period


def averaged_taps(filter_bank, period):
    width = TAPS + AVG - 1
    padded = jnp.pad(filter_bank, ((0, 0), (0, 0), (AVG - 1, AVG - 1)))
    total = padded[:, :, 0:width]
    for shift in range(1, AVG):
        total = total + padded[:, :, shift : shift + width]
    real, imag = total[0] * (1.0 / AVG), total[1] * (1.0 / AVG)
    to_real = jnp.stack([real, -imag], axis=-1).reshape(-1, 2 * width)
    to_imag = jnp.stack([imag, real], axis=-1).reshape(-1, 2 * width)
    to_real = jnp.pad(to_real, ((0, 0), (0, period - 2 * width)))
    to_imag = jnp.pad(to_imag, ((0, 0), (0, period - 2 * width)))
    return jnp.stack([to_real, jnp.roll(to_imag, -AVG, axis=1)], axis=1)


def build_bands(taps_ref, flag_ref, band_ref, block_rows):
    out_count, side_rows, local_rows, period = row_plan(block_rows)
    total_rows = 2 * side_rows + local_rows
    flags = flag_ref[...].astype(jnp.float32)

    def one_filter(f, carry):
        base = jnp.concatenate([taps_ref[f]] * 4, axis=0)
        tile = pltpu.roll(base, 0, 1, stride=AVG, stride_axis=0)
        start = 0
        for first, rows in (
            (-2 * SIDE, side_rows),
            (0, local_rows),
            (2 * out_count, side_rows),
        ):
            shifts = [(AVG * (first + row) - 2 * HALF) % period for row in range(0, rows, 8)]
            tiles = [pltpu.roll(tile, shift, 1)[:, : 2 * block_rows] for shift in shifts]
            band = jnp.concatenate(tiles, axis=0) * flags
            high = band.astype(jnp.bfloat16)
            low = (band - high.astype(jnp.float32)).astype(jnp.bfloat16)
            band_ref[f, start : start + rows, :] = high
            band_ref[f, total_rows + start : total_rows + start + rows, :] = low
            start += rows
        return carry

    lax.fori_loop(0, taps_ref.shape[0], one_filter, 0, unroll=4)


def band_kernel(taps_ref, flag_ref, band_ref, *, block_rows):
    build_bands(taps_ref, flag_ref, band_ref, block_rows)


def band_call(taps, flags):
    block_rows = flags.shape[1] // 2
    _, side_rows, local_rows, _ = row_plan(block_rows)
    return pl.pallas_call(
        functools.partial(band_kernel, block_rows=block_rows),
        in_specs=[pl.BlockSpec(memory_space=pltpu.VMEM)] * 2,
        out_specs=pl.BlockSpec(memory_space=pltpu.VMEM),
        out_shape=jax.ShapeDtypeStruct(
            (taps.shape[0], 2 * (2 * side_rows + local_rows), 2 * block_rows), jnp.bfloat16
        ),
    )(taps, flags)


def stream_kernel(
    index_ref,
    band_ref,
    vis_ref,
    out_ref,
    slab_ref,
    to_left,
    to_right,
    from_left,
    from_right,
    local_ref,
    sum_ref,
    done_ref,
    load_sem,
    left_send,
    right_send,
    left_recv,
    right_recv,
    done_send,
    done_recv,
    *,
    count,
):
    me = lax.axis_index("tm")
    _, block_rows, group, _, channels = slab_ref.shape
    chunks = done_ref.shape[0]
    per_owner = chunks // count
    out_count, side_rows, local_rows, _ = row_plan(block_rows)
    total_rows = 2 * side_rows + local_rows
    side = 2 * SIDE
    has_left, has_right = me > 0, me < count - 1

    def chunk_at(step):
        turn = step % count
        owner = (turn % 2) * (count - 1 - turn // 2) + (1 - turn % 2) * (turn // 2)
        return owner, step // count

    def load(step):
        owner, part = chunk_at(step)
        first = (owner * per_owner + part) * group
        slot = step % 2
        return pltpu.make_async_copy(
            vis_ref.at[:, pl.ds(first, group)], slab_ref.at[slot], load_sem.at[slot]
        )

    def remote(source, target, send_sem, recv_sem, device):
        return pltpu.make_async_remote_copy(
            src_ref=source,
            dst_ref=target,
            send_sem=send_sem,
            recv_sem=recv_sem,
            device_id={"tm": device},
            device_id_type=pl.DeviceIdType.MESH,
        )

    def leftward(step):
        return remote(
            to_left.at[step],
            from_right.at[step],
            left_send.at[step],
            right_recv.at[step],
            jnp.maximum(me - 1, 0),
        )

    def rightward(step):
        return remote(
            to_right.at[step],
            from_left.at[step],
            right_send.at[step],
            left_recv.at[step],
            jnp.minimum(me + 1, count - 1),
        )

    def placed(source, part):
        return out_ref.at[pl.ds(source * out_count, out_count), pl.ds(part * group, group)]

    def deliver(step):
        owner, part = chunk_at(step)
        return remote(
            done_ref.at[step], placed(me, part), done_send.at[step], done_recv.at[me, part], owner
        )

    def keep(step):
        _, part = chunk_at(step)
        return pltpu.make_async_copy(done_ref.at[step], placed(me, part), done_send.at[step])

    load(0).start()
    barrier = pltpu.get_barrier_semaphore()
    for offset in range(1, count):
        pl.semaphore_signal(
            barrier,
            inc=1,
            device_id={"tm": lax.rem(me + offset, count)},
            device_id_type=pl.DeviceIdType.MESH,
        )
    pl.semaphore_wait(barrier, count - 1)

    def compute(step, carry):
        @pl.when(step + 1 < chunks)
        def _():
            load(step + 1).start()

        load(step).wait()
        owner, part = chunk_at(step)
        first = (owner * per_owner + part) * group
        slot = step % 2
        for i in range(group):
            which = index_ref[first + i]
            slab = slab_ref[slot, :, i].reshape(2 * block_rows, channels)
            both = jnp.dot(band_ref[which], slab, preferred_element_type=jnp.float32)
            rows = both[:total_rows] + both[total_rows:]
            to_left[step, side * i : side * (i + 1), :] = rows[:side]
            local_ref[step, i] = rows[side_rows : side_rows + 2 * out_count]
            start = side_rows + local_rows
            to_right[step, side * i : side * (i + 1), :] = rows[start : start + side]

        @pl.when(has_left)
        def _():
            leftward(step).start()

        @pl.when(has_right)
        def _():
            rightward(step).start()

        return carry

    lax.fori_loop(0, chunks, compute, 0)

    def finish(step, carry):
        @pl.when(has_left)
        def _():
            rightward(step).wait_recv()

        @pl.when(has_right)
        def _():
            leftward(step).wait_recv()

        for i in range(group):
            sum_ref[...] = local_ref[step, i]

            @pl.when(has_left)
            def _():
                sum_ref[:side] += from_left[step, side * i : side * (i + 1), :]

            @pl.when(has_right)
            def _():
                sum_ref[2 * out_count - side :] += from_right[step, side * i : side * (i + 1), :]

            done_ref[step, :, i] = (
                sum_ref[...].astype(jnp.bfloat16).reshape(out_count, 2, channels)
            )
        owner, _ = chunk_at(step)

        @pl.when(owner == me)
        def _():
            keep(step).start()

        @pl.when(owner != me)
        def _():
            deliver(step).start()

        return carry

    lax.fori_loop(0, chunks, finish, 0)

    def drain(step, carry):
        @pl.when(has_left)
        def _():
            leftward(step).wait_send()

        @pl.when(has_right)
        def _():
            rightward(step).wait_send()

        owner, _ = chunk_at(step)

        @pl.when(owner == me)
        def _():
            keep(step).wait()

        @pl.when(owner != me)
        def _():
            deliver(step).wait_send()

        return carry

    lax.fori_loop(0, chunks, drain, 0)

    def collect(turn, carry):
        source = lax.rem(me + 1 + turn, count)
        for part in range(per_owner):
            remote(
                done_ref.at[0],
                placed(source, part),
                done_send.at[0],
                done_recv.at[source, part],
                source,
            ).wait_recv()
        return carry

    lax.fori_loop(0, count - 1, collect, 0)


def stream_call(kernel_index, bands, visibilities):
    block_rows, bases, _, channels = visibilities.shape
    count = lax.axis_size("tm")
    out_count = block_rows // AVG
    owned = bases // count
    group = GROUP
    while owned % group:
        group //= 2
    chunks = bases // group
    edge = pltpu.VMEM((chunks, 2 * SIDE * group, channels), jnp.float32)
    chunk_sems = pltpu.SemaphoreType.DMA((chunks,))
    return pl.pallas_call(
        functools.partial(stream_kernel, count=count),
        in_specs=[
            pl.BlockSpec(memory_space=pltpu.SMEM),
            pl.BlockSpec(memory_space=pltpu.VMEM),
            pl.BlockSpec(memory_space=pl.ANY),
        ],
        out_specs=pl.BlockSpec(memory_space=pl.ANY),
        out_shape=jax.ShapeDtypeStruct((count * out_count, owned, 2, channels), jnp.bfloat16),
        scratch_shapes=[
            pltpu.VMEM((2, block_rows, group, 2, channels), jnp.bfloat16),
            edge,
            edge,
            edge,
            edge,
            pltpu.VMEM((chunks, group, 2 * out_count, channels), jnp.float32),
            pltpu.VMEM((2 * out_count, channels), jnp.float32),
            pltpu.VMEM((chunks, out_count, group, 2, channels), jnp.bfloat16),
            pltpu.SemaphoreType.DMA((2,)),
            chunk_sems,
            chunk_sems,
            chunk_sems,
            chunk_sems,
            chunk_sems,
            pltpu.SemaphoreType.DMA((count, owned // group)),
        ],
        compiler_params=pltpu.CompilerParams(
            collective_id=0, has_side_effects=True, vmem_limit_bytes=50 * 1024 * 1024
        ),
    )(kernel_index, bands, visibilities)


def per_device(visibilities, flag_mask, kernel_index, filter_bank):
    period = row_plan(visibilities.shape[0])[3]
    taps = averaged_taps(filter_bank, period)
    flags = jnp.repeat(flag_mask, 2)[None, :]
    bands = band_call(taps, flags)
    return stream_call(kernel_index, bands, visibilities)


def solution(mesh):
    placed = (
        P(("group", "tm"), ("bl", "pol"), None, None),
        P(("group", "tm")),
        P(("bl", "pol")),
        P(),
    )
    return jax.shard_map(
        per_device,
        mesh=mesh,
        in_specs=placed,
        out_specs=P("group", ("bl", "pol", "tm"), None, None),
        check_vma=False,
    )
```
